32 devices in a mesh: fsdp: 8 (over y, x, core), tensor: 4 (over z).
Axes of the slice: x: 2, y: 2, z: 4, core: 2. Of those that a mesh axis runs over, the one named last changes fastest.
Arguments:
- layer_input: bfloat16 [8192, 2048], P(('fsdp', 'tensor')), may hold values from -6 to 6
- attn_gain: float32 [2048], P(('fsdp', 'tensor')), may hold values from 0.5 to 1.5
- attn_bias: float32 [2048], P(('fsdp', 'tensor')), may hold values from -1.75 to 1.75
- query_weight: bfloat16 [2048, 2048], P('fsdp', 'tensor'), may hold values from -0.125 to 0.125
- key_weight: bfloat16 [2048, 2048], P('fsdp', 'tensor'), may hold values from -0.125 to 0.125
- value_weight: bfloat16 [2048, 4096], P('fsdp', 'tensor'), may hold values from -0.125 to 0.125
- swish_weight: bfloat16 [2048, 4096], P('fsdp', 'tensor'), may hold values from -0.125 to 0.125
- output_weight: bfloat16 [2048, 4096], P('fsdp', 'tensor'), may hold values from -0.1875 to 0.1875
- ffn_gain: float32 [2048], P(('fsdp', 'tensor')), may hold values from 0.5 to 1.5
- ffn_bias: float32 [2048], P(('fsdp', 'tensor')), may hold values from -1.75 to 1.75
- gate_weight: bfloat16 [2048, 4096], P('fsdp', 'tensor'), may hold values from -0.125 to 0.125
- up_weight: bfloat16 [2048, 4096], P('fsdp', 'tensor'), may hold values from -0.125 to 0.125
- down_weight: bfloat16 [2048, 4096], P('fsdp', 'tensor'), may hold values from -0.1875 to 0.1875
- out_cotangent: bfloat16 [8192, 2048], P(('fsdp', 'tensor')), may hold values from -6 to 6
Outputs:
- layer_output: bfloat16 [8192, 2048], P(('fsdp', 'tensor'))
- input_grad: bfloat16 [8192, 2048], P(('fsdp', 'tensor'))
- attn_gain_grad: float32 [2048], P(('fsdp', 'tensor'))
- attn_bias_grad: float32 [2048], P(('fsdp', 'tensor'))
- query_grad: float32 [2048, 2048], P('fsdp', 'tensor')
- key_grad: float32 [2048, 2048], P('fsdp', 'tensor')
- value_grad: float32 [2048, 4096], P('fsdp', 'tensor')
- swish_grad: float32 [2048, 4096], P('fsdp', 'tensor')
- output_grad: float32 [2048, 4096], P('fsdp', 'tensor')
- ffn_gain_grad: float32 [2048], P(('fsdp', 'tensor'))
- ffn_bias_grad: float32 [2048], P(('fsdp', 'tensor'))
- gate_grad: float32 [2048, 4096], P('fsdp', 'tensor')
- up_grad: float32 [2048, 4096], P('fsdp', 'tensor')
- down_grad: float32 [2048, 4096], P('fsdp', 'tensor')
The draws below stay inside these ranges and needn't reach their ends.
All inputs are finite; a program needn't handle non-finite values.
Results may differ from the reference program's by a relative error of at most 0.019.
Values may be sent and summed in bfloat16 or wider, within the bound.
A program may use at most 192 MiB of HBM per device.

```python
import jax
import jax.numpy as jnp
from jax import lax

D = 2048
HEADS = 8
KEY_HEAD = 256
VAL_HEAD = 512
FF = 4096
BLOCK = 512
QK = 2048
VALUE = 4096
SEQ_LEN = 1024
TOKENS = 8192


def block_levels(key, dims, cuts, low, top_value):
    def one(axis_at, parts):
        heights = jax.random.uniform(jax.random.fold_in(jax.random.fold_in(key, 6), axis_at), (parts,), jnp.float32, low / len(cuts), top_value / len(cuts))
        return jnp.repeat(jnp.exp(heights), dims[axis_at] // parts).reshape((-1,) + (1,) * (len(dims) - axis_at - 1))

    factor_of = one(*cuts[0])
    for cut in cuts[1:]:
        factor_of = factor_of * one(*cut)
    return factor_of


def gaussian(stream_key, shape, scale, limit, shards=(), kind=jnp.bfloat16):
    level = block_levels(stream_key, shape, shards, -0.22, 0.18) if shards else 1.0
    entries = jax.random.normal(stream_key, shape, jnp.float32) * scale * level
    return jnp.minimum(jnp.maximum(entries, -limit), limit).astype(kind)


def setup_inputs(seed: int = 0) -> dict:
    key_of = jax.random.split(jax.random.key(seed), 15)
    return {
        "layer_input": gaussian(key_of[0], (TOKENS, D), 1.0, 6.0, ((0, 32),)),
        "attn_gain": jnp.clip(1.0 + 0.1 * jax.random.normal(key_of[1], (D,), jnp.float32), 0.5, 1.5),
        "attn_bias": gaussian(key_of[2], (D,), 0.3, 1.75, ((0, 32),), jnp.float32),
        "query_weight": gaussian(key_of[3], (D, QK), D ** -0.5, 0.125, ((0, 8), (1, 4))),
        "key_weight": gaussian(key_of[4], (D, QK), D ** -0.5, 0.125, ((0, 8), (1, 4))),
        "value_weight": gaussian(key_of[5], (D, VALUE), D ** -0.5, 0.125, ((0, 8), (1, 4))),
        "swish_weight": gaussian(key_of[6], (D, VALUE), D ** -0.5, 0.125, ((0, 8), (1, 4))),
        "output_weight": gaussian(key_of[7], (D, VALUE), (VALUE // 4) ** -0.5, 0.1875, ((0, 8), (1, 4))),
        "ffn_gain": jnp.clip(1.0 + 0.1 * jax.random.normal(key_of[8], (D,), jnp.float32), 0.5, 1.5),
        "ffn_bias": gaussian(key_of[9], (D,), 0.3, 1.75, ((0, 32),), jnp.float32),
        "gate_weight": gaussian(key_of[10], (D, FF), D ** -0.5, 0.125, ((0, 8), (1, 4))),
        "up_weight": gaussian(key_of[11], (D, FF), D ** -0.5, 0.125, ((0, 8), (1, 4))),
        "down_weight": gaussian(key_of[12], (D, FF), (FF // 4) ** -0.5, 0.1875, ((0, 8), (1, 4))),
        "out_cotangent": gaussian(key_of[13], (TOKENS, D), 1.0, 6.0, ((0, 32),)),
    }


@jax.custom_vjp
def low(v):
    return lax.optimization_barrier(v.astype(jnp.bfloat16)).astype(jnp.float32)

@jax.custom_vjp
def low_back(v):
    return v

def low_keep(v):
    return (low(v), None)

def low_pass(kept, grad):
    return (grad,)

def back_keep(v):
    return (v, None)

def back_low(kept, grad):
    return (low(grad),)
low.defvjp(low_keep, low_pass)
low_back.defvjp(back_keep, back_low)
epsilon = 1e-05
group_epsilon = 0.25
highest_precision_mode = lax.Precision.HIGHEST

def product_hi(left_side, right_side):
    return jnp.dot(left_side, right_side, precision=highest_precision_mode)

def layer_norm(stacked, gain_vec, bias_vec):
    average = lax.optimization_barrier(jnp.mean(stacked, axis=-1, keepdims=True))
    centred = stacked - average
    variance = lax.optimization_barrier(jnp.mean(centred * centred, axis=-1, keepdims=True))
    return centred * lax.rsqrt(variance + epsilon) * gain_vec + bias_vec

def rotation_tables(length, kind):
    half_width = KEY_HEAD // 2
    frequency = jnp.exp(-jnp.log(10000.0) * jnp.arange(half_width, dtype=jnp.float32) / half_width)
    angles = jnp.arange(length, dtype=jnp.float32)[:, None] * frequency[None, :]
    cosine_table = jnp.concatenate([jnp.cos(angles), jnp.cos(angles)], axis=-1).astype(kind)
    sine_table = jnp.concatenate([jnp.sin(angles), jnp.sin(angles)], axis=-1).astype(kind)
    return (cosine_table, sine_table)

def rotate(stacked, cosine_table, sine_table):
    first_half, second_half = jnp.split(stacked, 2, axis=-1)
    turned = jnp.concatenate([-second_half, first_half], axis=-1)
    return stacked * cosine_table[:, None, :] + turned * sine_table[:, None, :]

def decay_tables(kind):
    heads_index = jnp.arange(HEADS, dtype=jnp.float32)
    log_gamma = jnp.log1p(-jnp.exp2(-5.0 - heads_index))
    offsets = jnp.arange(BLOCK, dtype=jnp.float32)
    distance = offsets[:, None] - offsets[None, :]
    causal = distance >= 0
    decay_mask = jnp.where(causal[None], jnp.exp(jnp.where(causal, distance, 0.0)[None] * log_gamma[:, None, None]), 0.0)
    cross_scale = jnp.exp((offsets[:, None] + 1.0) * log_gamma[None, :])
    key_scale = jnp.exp((BLOCK - 1.0 - offsets[:, None]) * log_gamma[None, :])
    block_decay = jnp.exp(BLOCK * log_gamma)
    return (decay_mask.astype(kind), cross_scale.astype(kind), key_scale.astype(kind), block_decay.astype(kind))

def sequence_layer(single, params):
    attn_gain, attn_bias, query_weight, key_weight, value_weight, swish_weight, output_weight, ffn_gain, ffn_bias, gate_weight, up_weight, down_weight = params
    kind = single.dtype
    length = single.shape[0]
    blocks = length // BLOCK
    cosine_table, sine_table = rotation_tables(length, kind)
    decay_mask, cross_scale, key_scale, block_decay = decay_tables(kind)
    normed_one = low(layer_norm(single, attn_gain, attn_bias))
    query_pre = low_back(product_hi(normed_one, query_weight)).reshape(length, HEADS, KEY_HEAD)
    key_pre = low_back(product_hi(normed_one, key_weight)).reshape(length, HEADS, KEY_HEAD)
    values = low(low_back(product_hi(normed_one, value_weight))).reshape(length, HEADS, VAL_HEAD)
    swish_pre = low_back(product_hi(normed_one, swish_weight))
    query_rot = low(rotate(query_pre, cosine_table, sine_table))
    key_rot = rotate(key_pre, cosine_table, sine_table) * KEY_HEAD ** (-0.5)
    key_low = low(key_rot)
    key_dec = low(key_rot.reshape(blocks, BLOCK, HEADS, KEY_HEAD) * key_scale[None, :, :, None])

    def to_blocks(stacked):
        return stacked.reshape(blocks, BLOCK, HEADS, stacked.shape[-1])

    def block_step(state_now, pieces):
        block_query_rows, block_key_rows, block_decay_factors, block_value_rows = pieces
        attention_scores = low_back(jnp.einsum('yzk,nzk->zyn', block_query_rows, block_key_rows, precision=highest_precision_mode))
        weights = low(attention_scores * decay_mask)
        inner_term = low_back(jnp.einsum('him,mhe->ihe', weights, block_value_rows, precision=highest_precision_mode))
        cross_term = low_back(jnp.einsum('ihd,hde->ihe', block_query_rows, low(state_now), precision=highest_precision_mode))
        state_increment = low_back(jnp.einsum('xbz,xbl->bzl', block_decay_factors, block_value_rows, precision=highest_precision_mode))
        return (block_decay[:, None, None] * state_now + state_increment, inner_term + cross_scale[:, :, None] * cross_term)
    initial = jnp.zeros((HEADS, KEY_HEAD, VAL_HEAD), kind)
    _, retained = lax.scan(jax.checkpoint(block_step), initial, (to_blocks(query_rot), to_blocks(key_low), key_dec, to_blocks(values)))
    retained = retained.reshape(length, HEADS, VAL_HEAD)
    average = lax.optimization_barrier(jnp.mean(retained, axis=-1, keepdims=True))
    centred = retained - average
    spread = lax.optimization_barrier(jnp.mean(centred * centred, axis=-1, keepdims=True))
    group_normal = (centred * lax.rsqrt(spread + group_epsilon)).reshape(length, HEADS * VAL_HEAD)
    gated_rows = low(jax.nn.silu(swish_pre) * group_normal)
    hidden = single + low_back(product_hi(gated_rows, output_weight.T))
    normed_two = low(layer_norm(hidden, ffn_gain, ffn_bias))
    gate_pre = low_back(product_hi(normed_two, gate_weight))
    up_pre = low_back(product_hi(normed_two, up_weight))
    product = low(jax.nn.gelu(gate_pre, approximate=True) * up_pre)
    return hidden + low_back(product_hi(product, down_weight.T))

def reference(layer_input, attn_gain, attn_bias, query_weight, key_weight, value_weight, swish_weight, output_weight, ffn_gain, ffn_bias, gate_weight, up_weight, down_weight, out_cotangent):
    inputs = layer_input.astype(jnp.float32)
    kind = inputs.dtype
    params = jax.tree.map(lambda member: member.astype(kind), (attn_gain, attn_bias, query_weight, key_weight, value_weight, swish_weight, output_weight, ffn_gain, ffn_bias, gate_weight, up_weight, down_weight))

    def forward(source, weights_all):
        sequences = source.reshape(-1, SEQ_LEN, D)
        outputs = lax.map(lambda single: sequence_layer(single, weights_all), sequences)
        return outputs.reshape(-1, D)
    result, pullback = jax.vjp(forward, inputs, params)
    grad_in, grad_all = pullback(out_cotangent.astype(kind))
    return (result.astype(jnp.bfloat16), grad_in.astype(jnp.bfloat16), grad_all[0], grad_all[1], grad_all[2], grad_all[3], grad_all[4], grad_all[5], grad_all[6], grad_all[7], grad_all[8], grad_all[9], grad_all[10], grad_all[11])
```

```python
from functools import partial

import jax
import jax.numpy as jnp
from jax import lax
from jax.experimental import pallas as pl
from jax.experimental.pallas import tpu as pltpu
from jax.sharding import PartitionSpec as P

KEY_HEAD = 256
VAL_HEAD = 512
BLOCK = 512
HALF = KEY_HEAD // 2


epsilon = 1e-05
group_epsilon = 0.25
AXES = ("fsdp", "tensor")
F32 = jnp.float32
BF16 = jnp.bfloat16


def normalize(stacked, floor_value=epsilon):
    average = jnp.mean(stacked, axis=-1, keepdims=True)
    centred = stacked - average
    inverse = lax.rsqrt(jnp.mean(centred * centred, axis=-1, keepdims=True) + floor_value)
    return (centred * inverse, inverse)


def standardize_back(upstream, normal, inverse):
    return inverse * (
        upstream
        - jnp.mean(upstream, axis=-1, keepdims=True)
        - normal * jnp.mean(upstream * normal, axis=-1, keepdims=True)
    )


def norm_backward(upstream, normal, inverse, gain_vec):
    passed = standardize_back(upstream * gain_vec, normal, inverse)
    return (passed, jnp.sum(upstream * normal, axis=0), jnp.sum(upstream, axis=0))


def dot_nn(a, b):
    return jnp.dot(a, b, preferred_element_type=F32)


def dot_tn(a, b):
    return lax.dot_general(a, b, (((0,), (0,)), ((), ())), preferred_element_type=F32)


def dot_nt(a, b):
    return lax.dot_general(a, b, (((1,), (1,)), ((), ())), preferred_element_type=F32)


def rope(v, cos, sin):
    a, b = v[:, :HALF], v[:, HALF:]
    return jnp.concatenate([a * cos - b * sin, b * cos + a * sin], axis=1)


def rope_back(v, cos, sin):
    a, b = v[:, :HALF], v[:, HALF:]
    return jnp.concatenate([a * cos + b * sin, b * cos - a * sin], axis=1)


def rotate_kernel(q_ref, k_ref, v_ref, cos_ref, sin_ref, ks_ref, qo, ko, kd, inc):
    cos, sin = cos_ref[...], sin_ref[...]
    qo[...] = rope(q_ref[...], cos, sin).astype(BF16)
    key_rot = rope(k_ref[...], cos, sin) * KEY_HEAD**-0.5
    ko[...] = key_rot.astype(BF16)
    dec = (key_rot * ks_ref[...]).astype(BF16)
    kd[...] = dec
    inc[...] = dot_tn(dec, v_ref[...]).astype(BF16)


def forward_kernel(q_ref, k_ref, v_ref, s_ref, mask_ref, cs_ref, sw_ref, gated, normal, inv):
    scores = dot_nt(q_ref[...], k_ref[...])
    weights = (scores * mask_ref[...]).astype(BF16)
    kept = dot_nn(weights, v_ref[...]) + cs_ref[...] * dot_nn(q_ref[...], s_ref[...])
    norm, inverse = normalize(kept, group_epsilon)
    normal[...] = norm
    inv[...] = inverse
    gated[...] = (jax.nn.silu(sw_ref[...]) * norm).astype(BF16)


def backward_kernel(
    dg_ref, sw_ref, normal_ref, inv_ref, q_ref, k_ref, v_ref, s_ref, mask_ref, cs_ref,
    cos_ref, sin_ref, sl, ql, dkp, dvp, dso,
):
    dg, sw, normal = dg_ref[...], sw_ref[...], normal_ref[...]
    sig = jax.nn.sigmoid(sw)
    silu = sw * sig
    sl[...] = (dg * normal * (sig + silu * (1.0 - sig))).astype(BF16)
    dret = standardize_back(dg * silu, normal, inv_ref[...])
    inner = dret.astype(BF16)
    cross = (cs_ref[...] * dret).astype(BF16)
    q, k = q_ref[...], k_ref[...]
    dso[...] = dot_tn(q, cross).astype(BF16)
    mask = mask_ref[...]
    weights = (dot_nt(q, k) * mask).astype(BF16)
    dscore = (dot_nt(inner, v_ref[...]) * mask).astype(BF16)
    dvp[...] = dot_tn(weights, inner)
    dkp[...] = dot_tn(dscore, q)
    dq = dot_nn(dscore, k) + dot_nt(cross, s_ref[...])
    ql[...] = rope_back(dq, cos_ref[...], sin_ref[...]).astype(BF16)


def finish_kernel(dkp_ref, dvp_ref, kd_ref, v_ref, ds_ref, ks_ref, cos_ref, sin_ref, kl, vl):
    ds = ds_ref[...]
    vl[...] = (dvp_ref[...] + dot_nn(kd_ref[...], ds)).astype(BF16)
    dk = dkp_ref[...] + dot_nt(v_ref[...], ds) * ks_ref[...]
    kl[...] = (rope_back(dk, cos_ref[...], sin_ref[...]) * KEY_HEAD**-0.5).astype(BF16)


def key_spec(shift=0):
    return pl.BlockSpec((BLOCK, KEY_HEAD), lambda s, h: (s, h + shift))


val_spec = pl.BlockSpec((BLOCK, VAL_HEAD), lambda s, h: (s, h))
table_spec = pl.BlockSpec((BLOCK, HALF), lambda s, h: (0, 0))
scale_spec = pl.BlockSpec((None, BLOCK, 1), lambda s, h: (h, 0, 0))
mask_spec = pl.BlockSpec((None, BLOCK, BLOCK), lambda s, h: (h, 0, 0))
state_spec = pl.BlockSpec((None, None, KEY_HEAD, VAL_HEAD), lambda s, h: (s, h, 0, 0))
inv_spec = pl.BlockSpec((None, BLOCK, 1), lambda s, h: (h, s, 0))


def call(kernel, name, seqs, heads, in_specs, outs, flops):
    return pl.pallas_call(
        kernel,
        name=name,
        grid=(seqs, heads),
        in_specs=in_specs,
        out_specs=[o[0] for o in outs],
        out_shape=[jax.ShapeDtypeStruct(o[1], o[2]) for o in outs],
        cost_estimate=pl.CostEstimate(
            flops=flops * seqs * heads, bytes_accessed=16 << 20, transcendentals=0
        ),
    )


class Exchange:
    def __init__(self, fsdp, tensor):
        assert tensor == 4 and fsdp % 8 == 0
        self.fsdp, self.tensor = fsdp, tensor
        self.bits = (fsdp // 2).bit_length() - 1
        assert 2 << self.bits == fsdp
        f, t = lax.axis_index("fsdp"), lax.axis_index("tensor")
        self.rest, self.c = f // 2, f % 2
        self.zh, self.zl = t // 2, t % 2

    def permute(self, a, target):
        pairs = []
        for f in range(self.fsdp):
            for t in range(self.tensor):
                to = target(f // 2, f % 2, t // 2, t % 2)
                if to is not None:
                    r, c, zh, zl = to
                    pairs.append((f * self.tensor + t, (r * 2 + c) * self.tensor + zh * 2 + zl))
        return lax.ppermute(a, AXES, pairs)

    def over_rest(self, a, bit):
        return self.permute(a, lambda r, c, zh, zl: (r ^ (1 << bit), c, zh, zl))

    def over_c(self, a):
        return self.permute(a, lambda r, c, zh, zl: (r, 1 - c, zh, zl))

    def over_zl(self, a):
        return self.permute(a, lambda r, c, zh, zl: (r, c, zh, 1 - zl))

    def over_zh(self, a):
        return self.permute(a, lambda r, c, zh, zl: (r, c, 1 - zh, zl))

    def up_zh(self, a):
        return self.permute(a, lambda r, c, zh, zl: (r, c, 1, zl) if zh == 0 else None)

    def down_zh(self, a):
        return self.permute(a, lambda r, c, zh, zl: (r, c, 0, zl) if zh == 1 else None)

    def relative(self, a):
        count = self.fsdp // 2
        size = a.shape[-1] // count
        parts = [
            lax.dynamic_slice_in_dim(a, (self.rest ^ j) * size, size, axis=a.ndim - 1)
            for j in range(count)
        ]
        return jnp.concatenate(parts, axis=-1)

    def gather_vector(self, a):
        for here, over in ((self.zl, self.over_zl), (self.zh, self.over_zh), (self.c, self.over_c)):
            b = over(a)
            a = jnp.where(
                here == 0, jnp.concatenate([a, b], axis=-1), jnp.concatenate([b, a], axis=-1)
            )
        for bit in range(self.bits):
            a = jnp.concatenate([a, self.over_rest(a, bit)], axis=-1)
        return a

    def reduce_vector(self, a):
        for bit in reversed(range(self.bits)):
            keep, send = jnp.split(a, 2, axis=-1)
            a = keep + self.over_rest(send, bit)
        for here, over in ((self.c, self.over_c), (self.zh, self.over_zh), (self.zl, self.over_zl)):
            low, high = jnp.split(a, 2, axis=-1)
            a = jnp.where(here == 0, low, high) + over(jnp.where(here == 0, high, low))
        return a

    def gather_tokens(self, a):
        z = self.over_zl(a)
        s = self.over_c(a)
        sz = self.over_c(z)
        return jnp.concatenate([a, z, s, sz], axis=0)

    def reduce_tokens(self, a):
        rows = a.shape[0] // 4
        r = self.over_c(a[2 * rows :]).astype(F32)
        send = (a[rows : 2 * rows].astype(F32) + r[rows:]).astype(BF16)
        z = self.over_zl(send)
        return a[:rows].astype(F32) + r[:rows] + z.astype(F32)

    def spread(self, own):
        def first(r, c, zh, zl):
            return (r, c, 1 - zh, zl) if c == zh else (r, 1 - c, zh, zl)

        def second(r, c, zh, zl):
            return (r, 1 - c, 1 - zh, zl) if c != zh else None

        return self.permute(own, first), self.permute(own, second)

    def chip_block(self, own, p1, p2):
        home = self.c == self.zh
        mine = jnp.where(home, own, p1)
        other = jnp.where(home, p1, p2)
        low = jnp.where(self.c == 0, mine, other)
        high = jnp.where(self.c == 0, other, mine)
        return jnp.concatenate([low, high], axis=0)

    def gather_rest(self, block, after=None):
        for bit in range(self.bits - 2):
            block = jnp.concatenate([block, self.over_rest(block, bit)], axis=0)
        lo, hi = self.bits - 2, self.bits - 1
        if after is not None:
            block, _ = lax.optimization_barrier((block, after))
        x = self.over_rest(block, lo)
        y = self.over_rest(block, hi)
        h = block.shape[0] // 2
        d1 = self.over_rest(y[:h], lo)
        d2 = self.over_rest(x[h:], hi)
        return jnp.concatenate([block, x, y, d1, d2], axis=0), x

    def reduce_weight(self, a):
        lo, hi = self.bits - 2, self.bits - 1
        b, x, y, d = jnp.split(a, 4, axis=0)
        h = d.shape[0] // 2
        r1 = self.over_rest(d[:h], lo)
        r2 = self.over_rest(d[h:], hi)
        x = jnp.concatenate([x[:h], x[h:] + r2], axis=0)
        y = jnp.concatenate([y[:h] + r1, y[h:]], axis=0)
        rx = self.over_rest(x, lo)
        ry = self.over_rest(y, hi)
        a = (b.astype(F32) + rx.astype(F32) + ry.astype(F32)).astype(BF16)
        for bit in reversed(range(self.bits - 2)):
            keep, send = jnp.split(a, 2, axis=0)
            a = keep + self.over_rest(send, bit)
        low, high = jnp.split(a, 2, axis=0)
        mine = jnp.where(self.c == 0, low, high)
        other = jnp.where(self.c == 0, high, low)
        home = self.c == self.zh

        def first(r, c, zh, zl):
            return (r, 1 - c, zh, zl) if c == zh else (r, c, 1 - zh, zl)

        def second(r, c, zh, zl):
            return (r, 1 - c, 1 - zh, zl) if c != zh else None

        p1 = self.permute(jnp.where(home, other, mine), first)
        p2 = self.permute(other, second)
        kept = jnp.where(home, mine.astype(F32), 0.0)
        return kept + p1.astype(F32) + p2.astype(F32)


def body(
    fsdp,
    tensor,
    layer_input,
    attn_gain,
    attn_bias,
    query_weight,
    key_weight,
    value_weight,
    swish_weight,
    output_weight,
    ffn_gain,
    ffn_bias,
    gate_weight,
    up_weight,
    down_weight,
    out_cotangent,
):
    ex = Exchange(fsdp, tensor)
    rows = layer_input.shape[0]
    assert 2 * rows == BLOCK
    heads = query_weight.shape[1] // KEY_HEAD
    seqs = 2
    tokens = seqs * BLOCK
    qk = heads * KEY_HEAD
    val = heads * VAL_HEAD

    vectors = jnp.stack([attn_gain, attn_bias, ffn_gain, ffn_bias])
    vectors = ex.gather_vector(vectors)
    gain_one, bias_one, gain_two, bias_two = vectors[0], vectors[1], vectors[2], vectors[3]

    groups = [
        jnp.concatenate([query_weight, key_weight], axis=1),
        value_weight,
        swish_weight,
        output_weight,
        jnp.concatenate([gate_weight, up_weight], axis=1),
        down_weight,
    ]
    full = []
    last_z = last_xy = None
    for own in groups:
        if last_z is not None:
            own, _ = lax.optimization_barrier((own, last_z))
        p1, p2 = ex.spread(own)
        last_z = p1
        w, last_xy = ex.gather_rest(ex.chip_block(own, p1, p2), last_xy)
        full.append(w)
    w_qk, w_v, w_s, w_o, w_gu, w_d = full
    ff = down_weight.shape[1]

    offsets = jnp.arange(rows, dtype=F32)
    zl = ex.zl.astype(F32)
    within = jnp.concatenate([zl * rows + offsets, (1.0 - zl) * rows + offsets])
    position = within + ex.zh.astype(F32) * BLOCK
    frequency = jnp.exp(-jnp.log(10000.0) * jnp.arange(HALF, dtype=F32) / HALF)
    angles = position[:, None] * frequency[None, :]
    cos, sin = jnp.cos(angles), jnp.sin(angles)
    head_index = (2 * ex.c + ex.zl) * heads + jnp.arange(heads, dtype=jnp.int32)
    log_gamma = jnp.log1p(-jnp.exp2(-5.0 - head_index.astype(F32)))
    distance = within[:, None] - within[None, :]
    causal = distance >= 0
    mask = jnp.where(
        causal[None],
        jnp.exp(jnp.where(causal, distance, 0.0)[None] * log_gamma[:, None, None]),
        0.0,
    )
    cross_scale = jnp.exp((within[None, :, None] + 1.0) * log_gamma[:, None, None])
    key_scale = jnp.exp((BLOCK - 1.0 - within[None, :, None]) * log_gamma[:, None, None])

    inputs = ex.relative(layer_input).astype(F32)
    dout = ex.relative(out_cotangent)
    normal_one, inverse_one = normalize(inputs)
    normed_one = ex.gather_tokens((normal_one * gain_one + bias_one).astype(BF16))
    qk_pre = dot_nn(normed_one, w_qk)
    values = dot_nn(normed_one, w_v).astype(BF16)
    state_shape = (seqs, heads, KEY_HEAD, VAL_HEAD)
    kk = BLOCK * KEY_HEAD * VAL_HEAD * 2
    query, key_low, key_dec, inc = call(
        rotate_kernel,
        "rotate",
        seqs,
        heads,
        [key_spec(), key_spec(heads), val_spec, table_spec, table_spec, scale_spec],
        [(key_spec(), (tokens, qk), BF16)] * 3 + [(state_spec, state_shape, BF16)],
        kk,
    )(qk_pre, qk_pre, values, cos, sin, key_scale)
    state = ex.up_zh(inc)
    swish_pre = dot_nn(normed_one, w_s)
    gated, group_normal, group_inverse = call(
        forward_kernel,
        "retain",
        seqs,
        heads,
        [key_spec(), key_spec(), val_spec, state_spec, mask_spec, scale_spec, val_spec],
        [
            (val_spec, (tokens, val), BF16),
            (val_spec, (tokens, val), F32),
            (inv_spec, (heads, tokens, 1), F32),
        ],
        4 * kk,
    )(query, key_low, values, state, mask, cross_scale, swish_pre)
    hidden = inputs + ex.reduce_tokens(dot_nt(gated, w_o).astype(BF16))
    normal_two, inverse_two = normalize(hidden)
    normed_two = ex.gather_tokens((normal_two * gain_two + bias_two).astype(BF16))
    gate_pre = dot_nn(normed_two, w_gu[:, :ff])
    up_pre = dot_nn(normed_two, w_gu[:, ff:])
    gelu_value, gelu_pull = jax.vjp(partial(jax.nn.gelu, approximate=True), gate_pre)
    product = (gelu_value * up_pre).astype(BF16)
    output = hidden + ex.reduce_tokens(dot_nt(product, w_d).astype(BF16))

    down_rows = ex.gather_tokens(dout)
    down_grad = ex.reduce_weight(dot_tn(down_rows, product).astype(BF16))
    product_grad = dot_nn(down_rows, w_d)
    gate_low = gelu_pull(product_grad * up_pre)[0].astype(BF16)
    up_low = (product_grad * gelu_value).astype(BF16)
    normed_grad = ex.reduce_tokens(
        (dot_nt(gate_low, w_gu[:, :ff]) + dot_nt(up_low, w_gu[:, ff:])).astype(BF16)
    )
    gate_grad = ex.reduce_weight(dot_tn(normed_two, gate_low).astype(BF16))
    up_grad = ex.reduce_weight(dot_tn(normed_two, up_low).astype(BF16))
    hidden_part, ffn_gain_part, ffn_bias_part = norm_backward(
        normed_grad, normal_two, inverse_two, gain_two
    )
    hidden_grad = dout.astype(F32) + hidden_part
    attn_rows = ex.gather_tokens(hidden_grad.astype(BF16))
    gated_grad = dot_nn(attn_rows, w_o)
    output_grad = ex.reduce_weight(dot_tn(attn_rows, gated).astype(BF16))
    swish_low, query_low, dk_part, dv_part, ds_out = call(
        backward_kernel,
        "unretain",
        seqs,
        heads,
        [val_spec, val_spec, val_spec, inv_spec, key_spec(), key_spec(), val_spec, state_spec,
         mask_spec, scale_spec, table_spec, table_spec],
        [
            (val_spec, (tokens, val), BF16),
            (key_spec(), (tokens, qk), BF16),
            (key_spec(), (tokens, qk), F32),
            (val_spec, (tokens, val), F32),
            (state_spec, state_shape, BF16),
        ],
        9 * kk,
    )(gated_grad, swish_pre, group_normal, group_inverse, query, key_low, values, state, mask,
      cross_scale, cos, sin)
    ds_in = ex.down_zh(ds_out)
    swish_grad = ex.reduce_weight(dot_tn(normed_one, swish_low).astype(BF16))
    query_grad = ex.reduce_weight(dot_tn(normed_one, query_low).astype(BF16))
    early = dot_nt(swish_low, w_s) + dot_nt(query_low, w_qk[:, :qk])
    key_grad_low, value_low = call(
        finish_kernel,
        "finish",
        seqs,
        heads,
        [key_spec(), val_spec, key_spec(), val_spec, state_spec, scale_spec, table_spec, table_spec],
        [(key_spec(), (tokens, qk), BF16), (val_spec, (tokens, val), BF16)],
        2 * kk,
    )(dk_part, dv_part, key_dec, values, ds_in, key_scale, cos, sin)
    value_grad = ex.reduce_weight(dot_tn(normed_one, value_low).astype(BF16))
    key_grad = ex.reduce_weight(dot_tn(normed_one, key_grad_low).astype(BF16))
    late = early + dot_nt(key_grad_low, w_qk[:, qk:]) + dot_nt(value_low, w_v)
    input_part = ex.reduce_tokens(late.astype(BF16))
    inputs_part, attn_gain_part, attn_bias_part = norm_backward(
        input_part, normal_one, inverse_one, gain_one
    )
    input_grad = hidden_grad + inputs_part
    parts = ex.reduce_vector(
        jnp.stack([attn_gain_part, attn_bias_part, ffn_gain_part, ffn_bias_part])
    )
    return (
        ex.relative(output.astype(BF16)),
        ex.relative(input_grad.astype(BF16)),
        parts[0],
        parts[1],
        query_grad,
        key_grad,
        value_grad,
        swish_grad,
        output_grad,
        parts[2],
        parts[3],
        gate_grad,
        up_grad,
        down_grad,
    )


def solution(mesh):
    rows = P(AXES, None)
    vector = P(AXES)
    weight = P("fsdp", "tensor")
    in_specs = (
        (rows, vector, vector) + (weight,) * 5 + (vector, vector) + (weight,) * 3 + (rows,)
    )
    out_specs = (
        (rows, rows, vector, vector) + (weight,) * 5 + (vector, vector) + (weight,) * 3
    )
    step = partial(body, mesh.shape["fsdp"], mesh.shape["tensor"])
    return jax.shard_map(step, mesh=mesh, in_specs=in_specs, out_specs=out_specs, check_vma=False)
```
